32 devices in a mesh: groups: 2 (over y), head: 4 (over z), state: 4 (over x, core).
Axes of the slice: x: 2, y: 2, z: 4, core: 2. Of those that a mesh axis runs over, the one named last changes fastest.
Arguments:
- tokens: bfloat16 [32, 2048], P(('groups', 'head'), 'state'), parts along dimension 0, may hold values from -20 to 20
- mixer_norm: float32 [2048], P('state'), may hold values from 0.1 to 1.9
- input_proj: bfloat16 [2, 2048, 8192], P(None, 'state', 'head'), may hold values from -0.125 to 0.125
- conv_weight: float32 [4, 8192], P(None, 'head'), may hold values from -3 to 3
- conv_bias: float32 [8192], P('head'), may hold values from -3 to 3
- conv_state: float32 [3, 32, 8192], P(None, 'groups', 'head'), parts along dimension 1, may hold values from -6 to 6
- state_proj: bfloat16 [8192, 288], P('head'), may hold values from -0.125 to 0.125
- step_gain: float32 [256], replicated, may hold values from 0.1 to 1.9
- step_proj: bfloat16 [256, 8192], P(None, 'head'), may hold values from -0.375 to 0.375
- step_bias: float32 [8192], P('head'), may hold values from -6 to -1
- decay_log: float32 [16, 8192], P('state', 'head'), may hold values from 0 to 2.77
- skip_gain: float32 [8192], P('head'), may hold values from 0.5 to 1.5
- ssm_state: float32 [16, 32, 8192], P('state', 'groups', 'head'), parts along dimension 1, may hold values from -6 to 6
- output_proj: bfloat16 [8192, 2048], P('head', 'state'), may hold values from -0.0625 to 0.0625
- moe_norm: float32 [2048], replicated, may hold values from 0.1 to 1.9
- router_weight: float32 [2048, 8], replicated, may hold values from -0.125 to 0.125
- expert_ids: int32 [32, 2], P(('groups', 'head')), parts along dimension 0, may hold values from 0 to 7, as said below
- slot_ids: int32 [32, 2], P(('groups', 'head')), parts along dimension 0, may hold values from 0 to 3, as said below
- gate_proj: bfloat16 [8, 2048, 7168], P('head', None, 'state'), may hold values from -0.125 to 0.125
- up_proj: bfloat16 [8, 2048, 7168], P('head', None, 'state'), may hold values from -0.125 to 0.125
- down_proj: bfloat16 [8, 7168, 2048], P('head', 'state'), may hold values from -0.0625 to 0.0625
Outputs:
- layer_out: bfloat16 [32, 2048], P(('groups', 'head'), 'state'), parts along dimension 0
- new_conv: float32 [3, 32, 8192], P(None, 'groups', 'head'), parts along dimension 1
- new_state: float32 [16, 32, 8192], P('state', 'groups', 'head'), parts along dimension 1
- expert_load: float32 [16], P('groups'), parts along dimension 0
- aux_loss: float32 [2], P('groups'), parts along dimension 0
The draws below stay inside these ranges and needn't reach their ends.
There are 2 independent parts, one for each index of `groups`. The reference program is written for one: setup_inputs(seed, part) draws one part's arguments, and reference() takes and returns one part's arrays. A program takes and returns all parts, laid end to end along the dimension named above; an argument that names none is the same for every part. Nothing has to cross between parts.
Inputs may be any that keep to these rules, and one draw needn't show every extreme that they name: `expert_ids`: each row names 2 different experts. One expert, the same on every device, is named by every row. `slot_ids`: among the choices of one aligned block of 4 rows that name one expert, the slot positions are distinct and run from 0 to their count less one.
All inputs are finite; a program needn't handle non-finite values.
Results may differ from the reference program's by a relative error of at most 0.007.
Values may be sent and summed in bfloat16 or wider, within the bound.
A program may use at most 128 MiB of HBM per device.

```python
import math
import jax
import jax.numpy as jnp
from jax import lax

D = 2048
D_INNER = 8192
D_STATE = 16
DT_RANK = 256
CONV = 4
EXPERTS = 8
TOPK = 2
FF = 7168
SEQ_DEV = 4
BATCH = 16
CAP = 2
SPLIT = 1
EXP_ROWS = 8
FF_PART = 7168


def routing_pair(key):
    base_key = jax.random.fold_in(key, 11)
    key_hot = jax.random.fold_in(base_key, 0)
    key_score = jax.random.fold_in(base_key, 2)
    key_prio = jax.random.fold_in(base_key, 3)
    blocks = BATCH // SEQ_DEV
    assigned = SEQ_DEV * TOPK
    hot_expert = jax.random.randint(key_hot, (), 0, EXPERTS)
    expert_score = jax.random.randint(key_score, (blocks, SEQ_DEV, EXPERTS), 0, 1 << 20) * EXPERTS + jnp.arange(EXPERTS, dtype=jnp.int32)
    is_hot = jnp.arange(EXPERTS, dtype=jnp.int32) == hot_expert
    expert_score = jnp.where(is_hot[None, None, :], expert_score + (1 << 30), expert_score)
    chosen_ids = lax.top_k(expert_score, TOPK)[1].astype(jnp.int32)
    flat_ids = chosen_ids.reshape(blocks, assigned)
    priority = jax.random.randint(key_prio, (blocks, assigned), 0, 1 << 20) * assigned + jnp.arange(assigned, dtype=jnp.int32)
    earlier = (flat_ids[:, :, None] == flat_ids[:, None, :]) & (priority[:, None, :] < priority[:, :, None])
    slot_pos = jnp.sum(earlier.astype(jnp.int32), axis=2)
    return (chosen_ids.reshape(BATCH, TOPK), slot_pos.reshape(BATCH, TOPK).astype(jnp.int32))


def draw_expert_ids(key, part):
    return routing_pair(key)[0]


def draw_slot_ids(key, part):
    return routing_pair(key)[1]


def draw_tokens(key, part):
    base_key = jax.random.fold_in(key, 5)
    key_scale, key_value = jax.random.split(base_key, 2)
    row_scale = jnp.exp(jax.random.uniform(key_scale, (BATCH, 1), jnp.float32, math.log(0.3), math.log(3.0)))
    values = jax.random.normal(key_value, (BATCH, D), jnp.float32)
    return jnp.clip(values * row_scale, -20.0, 20.0).astype(jnp.bfloat16)


def block_scale(rng, dims, cuts, low, top_value):
    def one(position, blocks):
        heights = jax.random.uniform(jax.random.fold_in(jax.random.fold_in(rng, 6), position), (blocks,), jnp.float32, low / len(cuts), top_value / len(cuts))
        return jnp.repeat(jnp.exp(heights), dims[position] // blocks).reshape((-1,) + (1,) * (len(dims) - position - 1))

    loudness = one(*cuts[0])
    for cut in cuts[1:]:
        loudness = loudness * one(*cut)
    return loudness


def noise(rng, shape, spread, most, cuts=(), held_as=jnp.bfloat16):
    entries = jax.random.normal(rng, shape, jnp.float32) * spread
    if len(cuts) > 0:
        entries = block_scale(rng, shape, cuts, -0.22, 0.18) * entries
    return jnp.clip(entries, min=-most, max=most).astype(held_as)


def setup_inputs(seed: int = 0, part: int = 0) -> dict:
    key_list = jax.random.split(jax.random.key(seed), 22)
    own_keys = jax.random.split(jax.random.fold_in(key_list[21], part), 22)
    return {
        "tokens": draw_tokens(jax.random.fold_in(jax.random.fold_in(key_list[21], part), 71), part),
        "mixer_norm": jnp.clip(1.0 + 0.18 * jax.random.normal(key_list[1], (D,), jnp.float32), 0.1, 1.9),
        "input_proj": noise(key_list[2], (2, D, D_INNER), D ** -0.5, 0.125, ((1, 4), (2, 4))),
        "conv_weight": noise(key_list[3], (CONV, D_INNER), CONV ** -0.5, 3.0, ((1, 4),), jnp.float32),
        "conv_bias": noise(key_list[4], (D_INNER,), 0.5, 3.0, ((0, 4),), jnp.float32),
        "conv_state": noise(own_keys[5], (CONV - 1, BATCH, D_INNER), 1.0, 6.0, ((2, 4),), jnp.float32),
        "state_proj": noise(key_list[6], (D_INNER, DT_RANK + 2 * D_STATE), (D_INNER // 4) ** -0.5, 0.125, ((0, 4),)),
        "step_gain": jnp.clip(1.0 + 0.18 * jax.random.normal(key_list[7], (DT_RANK,), jnp.float32), 0.1, 1.9),
        "step_proj": noise(key_list[8], (DT_RANK, D_INNER), DT_RANK ** -0.5, 0.375, ((1, 4),)),
        "step_bias": jnp.clip(-6.0 + 5.0 * jax.random.uniform(key_list[9], (D_INNER,), jnp.float32) ** block_scale(key_list[9], (D_INNER,), ((0, 4),), -0.2, 0.2), -6.0, -1.0),
        "decay_log": jnp.clip(2.77 * jax.random.uniform(key_list[10], (D_STATE, D_INNER), jnp.float32) ** block_scale(key_list[10], (D_STATE, D_INNER), ((0, 4), (1, 4)), -0.2, 0.2), 0.0, 2.77),
        "skip_gain": jnp.clip(0.5 + 1.0 * jax.random.uniform(key_list[11], (D_INNER,), jnp.float32) ** block_scale(key_list[11], (D_INNER,), ((0, 4),), -0.2, 0.2), 0.5, 1.5),
        "ssm_state": noise(own_keys[12], (D_STATE, BATCH, D_INNER), 1.0, 6.0, ((0, 4), (2, 4)), jnp.float32),
        "output_proj": noise(key_list[13], (D_INNER, D), D_INNER ** -0.5, 0.0625, ((0, 4), (1, 4))),
        "moe_norm": jnp.clip(1.0 + 0.18 * jax.random.normal(key_list[14], (D,), jnp.float32), 0.1, 1.9),
        "router_weight": noise(key_list[15], (D, EXPERTS), D ** -0.5, 0.125, (), jnp.float32),
        "expert_ids": draw_expert_ids(jax.random.fold_in(jax.random.fold_in(key_list[21], part), 71), part),
        "slot_ids": draw_slot_ids(jax.random.fold_in(jax.random.fold_in(key_list[21], part), 71), part),
        "gate_proj": noise(key_list[18], (EXP_ROWS, D, FF_PART), D ** -0.5, 0.125, ((0, 4), (2, 4))),
        "up_proj": noise(key_list[19], (EXP_ROWS, D, FF_PART), D ** -0.5, 0.125, ((0, 4), (2, 4))),
        "down_proj": noise(key_list[20], (EXP_ROWS, FF_PART, D), FF ** -0.5, 0.0625, ((0, 4), (1, 4))),
    }


def reference(tokens, mixer_norm, input_proj, conv_weight, conv_bias, conv_state, state_proj, step_gain, step_proj, step_bias, decay_log, skip_gain, ssm_state, output_proj, moe_norm, router_weight, expert_ids, slot_ids, gate_proj, up_proj, down_proj):
    tok_f32 = tokens.astype(jnp.float32)
    inv_first = lax.rsqrt(lax.optimization_barrier(jnp.mean(tok_f32 * tok_f32, axis=1, keepdims=True)) + 1e-05)
    normed = (tok_f32 * inv_first * mixer_norm).astype(jnp.bfloat16)
    conv_input = jnp.dot(normed, input_proj[0], preferred_element_type=jnp.float32)
    gate_branch = jnp.dot(normed, input_proj[1], preferred_element_type=jnp.float32)
    window = jnp.concatenate([conv_state, conv_input[None]], axis=0)
    conv_out = jax.nn.silu(lax.optimization_barrier(jnp.sum(conv_weight[:, None, :] * window, axis=0)) + conv_bias)
    new_conv = window[1:]
    projected = jnp.dot(conv_out.astype(jnp.bfloat16), state_proj, preferred_element_type=jnp.float32)
    step_low = projected[:, :DT_RANK]
    b_input = projected[:, DT_RANK:DT_RANK + D_STATE]
    c_output = projected[:, DT_RANK + D_STATE:]
    step_inv = lax.rsqrt(lax.optimization_barrier(jnp.mean(step_low * step_low, axis=1, keepdims=True)) + 1e-06)
    step_normed = (step_low * step_inv * step_gain).astype(jnp.bfloat16)
    step_size = jax.nn.softplus(jnp.dot(step_normed, step_proj, preferred_element_type=jnp.float32) + step_bias)
    decay_rate = jnp.exp(-step_size[None] * jnp.exp(decay_log)[:, None, :])
    new_state = decay_rate * ssm_state + step_size[None] * b_input.T[:, :, None] * conv_out[None]
    readout = lax.optimization_barrier(jnp.sum(c_output.T[:, :, None] * new_state, axis=0))
    mixer_act = ((readout + skip_gain * conv_out) * jax.nn.silu(gate_branch)).astype(jnp.bfloat16)
    residual = (tok_f32 + jnp.dot(mixer_act, output_proj, preferred_element_type=jnp.float32)).astype(jnp.bfloat16)
    resid_f32 = residual.astype(jnp.float32)
    inv_second = lax.rsqrt(lax.optimization_barrier(jnp.mean(resid_f32 * resid_f32, axis=1, keepdims=True)) + 1e-05)
    scaled = resid_f32 * moe_norm
    row_normed = (scaled * inv_second).astype(jnp.bfloat16)
    logits = inv_second * jnp.dot(scaled, router_weight, precision=lax.Precision.HIGHEST)
    expert_hit = expert_ids[:, :, None] == jnp.arange(EXPERTS, dtype=jnp.int32)[None, None, :]
    chosen = lax.optimization_barrier(jnp.sum(jnp.where(expert_hit, logits[:, None, :], 0.0), axis=2))
    gate_probs = jax.nn.sigmoid(chosen - chosen[:, ::-1])
    kept_mask = slot_ids < CAP
    mix_weight = jnp.where(kept_mask, gate_probs, 0.0)
    token_weight = lax.optimization_barrier(jnp.sum(jnp.where(expert_hit, mix_weight[:, :, None], 0.0), axis=1))
    gate_all = gate_proj.reshape(EXPERTS, SPLIT, D, FF_PART).transpose(0, 2, 1, 3).reshape(EXPERTS, D, SPLIT * FF_PART)
    up_all = up_proj.reshape(EXPERTS, SPLIT, D, FF_PART).transpose(0, 2, 1, 3).reshape(EXPERTS, D, SPLIT * FF_PART)
    down_all = down_proj.reshape(EXPERTS, SPLIT * FF_PART, D)

    def one_expert(carry, inputs):
        gate_one, up_one, down_one, weight_one = inputs
        gate_val = jnp.dot(row_normed, gate_one, preferred_element_type=jnp.float32)
        up_val = jnp.dot(row_normed, up_one, preferred_element_type=jnp.float32)
        hidden = (jax.nn.silu(gate_val) * up_val).astype(jnp.bfloat16)
        expert_value = jnp.dot(hidden, down_one, preferred_element_type=jnp.float32)
        return (carry + weight_one[:, None] * expert_value, None)
    expert_mix, _ = lax.scan(one_expert, jnp.zeros((BATCH, D), jnp.float32), (gate_all, up_all, down_all, token_weight.T))
    layer_out = (resid_f32 + expert_mix).astype(jnp.bfloat16)
    expert_load = lax.optimization_barrier(jnp.sum(jnp.where(expert_hit & kept_mask[:, :, None], 1.0, 0.0), axis=(0, 1))).astype(jnp.float32)
    mean_prob = lax.optimization_barrier(jnp.mean(jax.nn.sigmoid(logits), axis=0))
    aux_loss = (EXPERTS * jnp.sum(expert_load / (BATCH * TOPK) * mean_prob)).reshape(1)
    return (layer_out, new_conv, new_state, expert_load, aux_loss)
```

```python
import jax
import jax.numpy as jnp
from jax import lax
from jax.experimental import pallas as pl
from jax.experimental.pallas import tpu as pltpu
from jax.sharding import PartitionSpec as P

D = 2048
D_STATE = 16
DT_RANK = 256
EXPERTS = 8
TOPK = 2
CAP = 2


NORM_EPS = 1e-05
STEP_EPS = 1e-06
VMEM_BYTES = 67043328


def expert_ffn(received, gate_proj, up_proj, down_proj):
    gate_val = jnp.einsum("nlcd,ldf->nlcf", received, gate_proj, preferred_element_type=jnp.float32)
    up_val = jnp.einsum("nlcd,ldf->nlcf", received, up_proj, preferred_element_type=jnp.float32)
    hidden = (jax.nn.silu(gate_val) * up_val).astype(jnp.bfloat16)
    return jnp.einsum("nlcf,lfd->nlcd", hidden, down_proj, preferred_element_type=jnp.float32)


def per_device(
    tokens,
    mixer_norm,
    input_proj,
    conv_weight,
    conv_bias,
    conv_state,
    state_proj,
    step_gain,
    step_proj,
    step_bias,
    decay_log,
    skip_gain,
    ssm_state,
    output_proj,
    moe_norm,
    router_weight,
    expert_ids,
    slot_ids,
    gate_proj,
    up_proj,
    down_proj,
):
    head_count = lax.axis_size("head")
    state_index = lax.axis_index("state")
    own_rows = tokens.shape[0]
    tok_f32 = tokens.astype(jnp.float32)
    first_sq = lax.psum(jnp.sum(tok_f32 * tok_f32, axis=1), "state")
    inv_first = lax.rsqrt(first_sq / D + NORM_EPS)[:, None]
    normed = (tok_f32 * inv_first * mixer_norm).astype(jnp.bfloat16)
    branch_part = jnp.einsum(
        "td,kdc->ktc",
        lax.all_gather(normed, "head", axis=0, tiled=True),
        input_proj,
        preferred_element_type=jnp.float32,
    )
    branch_full = lax.psum(branch_part, "state")
    conv_input = branch_full[0]
    gate_branch = branch_full[1]
    window = jnp.concatenate([conv_state, conv_input[None]], axis=0)
    conv_out = jax.nn.silu(jnp.sum(conv_weight[:, None, :] * window, axis=0) + conv_bias)
    new_conv = window[1:]
    proj_part = jnp.dot(
        conv_out.astype(jnp.bfloat16), state_proj, preferred_element_type=jnp.float32
    )
    projected = lax.psum(proj_part, "head")
    step_low = projected[:, :DT_RANK]
    state_slab = decay_log.shape[0]
    b_input = lax.dynamic_slice_in_dim(projected, DT_RANK + state_index * state_slab, state_slab, 1)
    c_output = lax.dynamic_slice_in_dim(
        projected, DT_RANK + D_STATE + state_index * state_slab, state_slab, 1
    )
    step_inv = lax.rsqrt(jnp.mean(step_low * step_low, axis=1, keepdims=True) + STEP_EPS)
    step_normed = (step_low * step_inv * step_gain).astype(jnp.bfloat16)
    step_size = jax.nn.softplus(
        jnp.dot(step_normed, step_proj, preferred_element_type=jnp.float32) + step_bias
    )
    decay_rate = jnp.exp(-step_size[None] * jnp.exp(decay_log)[:, None, :])
    new_state = decay_rate * ssm_state + step_size[None] * b_input.T[:, :, None] * conv_out[None]
    read_part = jnp.sum(c_output.T[:, :, None] * new_state, axis=0)
    readout = lax.psum(read_part, "state")
    mixer_act = ((readout + skip_gain * conv_out) * jax.nn.silu(gate_branch)).astype(jnp.bfloat16)
    mixer_sum = lax.psum_scatter(
        jnp.dot(mixer_act, output_proj, preferred_element_type=jnp.float32),
        "head",
        scatter_dimension=0,
        tiled=True,
    )
    residual = (tok_f32 + mixer_sum).astype(jnp.bfloat16)
    full_rows = lax.all_gather(residual, "state", axis=1, tiled=True).astype(jnp.float32)
    inv_second = lax.rsqrt(jnp.mean(full_rows * full_rows, axis=1, keepdims=True) + NORM_EPS)
    scaled = full_rows * moe_norm
    logits = inv_second * jnp.dot(scaled, router_weight, precision=lax.Precision.HIGHEST)
    row_normed = (scaled * inv_second).astype(jnp.bfloat16)
    expert_hit = expert_ids[:, :, None] == jnp.arange(EXPERTS, dtype=jnp.int32)[None, None, :]
    chosen = jnp.sum(jnp.where(expert_hit, logits[:, None, :], 0.0), axis=2)
    gate_probs = jax.nn.sigmoid(chosen - chosen[:, ::-1])
    kept_mask = slot_ids < CAP
    mix_weight = jnp.where(kept_mask, gate_probs, 0.0)
    slot_hit = slot_ids[:, :, None] == jnp.arange(CAP, dtype=jnp.int32)[None, None, :]
    slot_place = expert_hit[:, :, :, None] & slot_hit[:, :, None, :]
    dispatch = jnp.sum(slot_place.astype(jnp.int32), axis=1).astype(jnp.bfloat16)
    combine_weight = jnp.sum(jnp.where(slot_place, mix_weight[:, :, None, None], 0.0), axis=1)
    outgoing = jnp.einsum(
        "tec,td->ecd", dispatch, row_normed, preferred_element_type=jnp.float32
    ).astype(jnp.bfloat16)
    row_width = outgoing.shape[2]
    local_experts = gate_proj.shape[0]
    expert_groups = EXPERTS // local_experts
    copies = head_count * local_experts // EXPERTS
    outgoing = jnp.broadcast_to(
        outgoing.reshape(expert_groups, 1, local_experts, CAP, row_width),
        (expert_groups, copies, local_experts, CAP, row_width),
    )
    outgoing = outgoing.reshape(head_count, local_experts, CAP, row_width)
    partial_out = expert_ffn(
        lax.all_to_all(outgoing, "head", split_axis=0, concat_axis=0, tiled=True),
        gate_proj,
        up_proj,
        down_proj,
    )
    returned = lax.all_to_all(
        partial_out.astype(jnp.bfloat16), "head", split_axis=0, concat_axis=0, tiled=True
    ).astype(partial_out.dtype)
    per_expert = returned.reshape(expert_groups, copies, local_experts, CAP, row_width).sum(axis=1)
    per_expert = per_expert.reshape(EXPERTS, CAP, row_width)
    expert_mix = jnp.einsum(
        "tec,ecd->td", combine_weight, per_expert, precision=lax.Precision.HIGHEST
    )
    expert_mix = lax.psum_scatter(
        expert_mix.astype(jnp.bfloat16), "state", scatter_dimension=1, tiled=True
    ).astype(jnp.float32)
    layer_out = (residual.astype(jnp.float32) + expert_mix).astype(jnp.bfloat16)
    load_own = jnp.sum(jnp.where(expert_hit & kept_mask[:, :, None], 1.0, 0.0), axis=(0, 1)).astype(
        jnp.float32
    )
    prob_own = jnp.sum(jax.nn.sigmoid(logits), axis=0)
    load_sum, prob_sum = lax.psum((load_own, prob_own), "head")
    total_rows = head_count * own_rows
    aux_value = EXPERTS * jnp.sum(load_sum / (total_rows * TOPK) * (prob_sum / total_rows))
    return (layer_out, new_conv, new_state, load_sum, aux_value.reshape(1))


def dot(left, right):
    return jnp.dot(left, right, preferred_element_type=jnp.float32)


def fused_kernel(dims, *refs):
    heads, states, own, local, split, slab = dims
    (pay, nrm, wi, cw, cb, cs, wsp, sg, wst, sb, dl, sk, ss, wo, mn, rw, wg, wu, wd) = refs[:19]
    (out, new_conv, new_state, load, aux) = refs[19:24]
    (v_nrm, v_wi, v_cw, v_cb, v_cs, v_wsp, v_sg, v_wst, v_sb, v_dl, v_sk, v_ss, v_wo, v_mn, v_rw, v_wg, v_wu, v_wd) = refs[24:42]
    (pay_buf, sq_buf, br_buf, pj_buf, rd_buf, ms_buf, rs_buf, xo_buf, xi_buf) = refs[42:51]
    (conv_in, conv_out, gate_act, resid, xn, hid, ld_sem, ex_sem, in_sem, h_send, h_recv, s_send, s_recv, x_send, x_recv, o_sem) = refs[51:]
    me_h = lax.axis_index("head")
    me_s = lax.axis_index("state")
    batch = pay.shape[0]
    width = v_nrm.shape[1]
    model = width * states
    chans = v_cb.shape[1]
    rank = v_sg.shape[1]
    experts = v_rw.shape[1]

    smalls = [(nrm, v_nrm), (cw, v_cw), (cb, v_cb), (cs, v_cs), (wsp, v_wsp), (sg, v_sg), (wst, v_wst), (sb, v_sb), (dl, v_dl), (sk, v_sk), (ss, v_ss), (wo, v_wo), (mn, v_mn), (rw, v_rw)]
    in_copies = [pltpu.make_async_copy(wi.at[k], v_wi.at[k], in_sem.at[k]) for k in range(2)]
    loads = [pltpu.make_async_copy(a, b, ld_sem.at[i]) for i, (a, b) in enumerate(smalls)]
    (l_nrm, l_cw, l_cb, l_cs, l_wsp, l_sg, l_wst, l_sb, l_dl, l_sk, l_ss, l_wo, l_mn, l_rw) = loads
    ex_copies = []
    for e in range(local):
        ex_copies.append([pltpu.make_async_copy(a.at[e], b.at[e], ex_sem.at[3 * e + j]) for j, (a, b) in enumerate(((wg, v_wg), (wu, v_wu), (wd, v_wd)))])
    l_nrm.start()
    for c in in_copies:
        c.start()
    for c in loads[1:]:
        c.start()

    barrier = pltpu.get_barrier_semaphore()
    for dh in range(heads):
        for ds in range(states):
            if dh or ds:
                pl.semaphore_signal(
                    barrier,
                    inc=1,
                    device_id={"head": lax.rem(me_h + dh, heads), "state": lax.rem(me_s + ds, states)},
                    device_id_type=pl.DeviceIdType.MESH,
                )
    pl.semaphore_wait(barrier, heads * states - 1)

    def head_send(step, source, dest):
        copies = []
        for d in range(1, heads):
            c = pltpu.make_async_remote_copy(
                src_ref=source,
                dst_ref=dest,
                send_sem=h_send.at[step, d],
                recv_sem=h_recv.at[step, d],
                device_id={"head": lax.rem(me_h + d, heads)},
                device_id_type=pl.DeviceIdType.MESH,
            )
            c.start()
            copies.append(c)
        return copies

    def state_send(step, source, dest):
        copies = []
        for d in range(1, states):
            c = pltpu.make_async_remote_copy(
                src_ref=source,
                dst_ref=dest,
                send_sem=s_send.at[step, d],
                recv_sem=s_recv.at[step, d],
                device_id={"state": lax.rem(me_s + d, states)},
                device_id_type=pl.DeviceIdType.MESH,
            )
            c.start()
            copies.append(c)
        return copies

    def recv(copies):
        for c in copies:
            c.wait_recv()

    pending = []
    c_pay = head_send(0, pay, pay_buf.at[me_h])
    pending += c_pay
    pay_buf[me_h] = pay[...]
    for group in ex_copies:
        for c in group:
            c.start()
    recv(c_pay)
    whole = pay_buf[0].astype(jnp.float32)
    for j in range(1, heads):
        whole = whole + pay_buf[j].astype(jnp.float32)
    tok = whole[:, :width]
    route = whole[:, width:]
    sq_buf[me_s] = jnp.broadcast_to(jnp.sum(tok * tok, axis=1, keepdims=True), sq_buf.shape[1:])
    c_sq = state_send(0, sq_buf.at[me_s], sq_buf.at[me_s])
    pending += c_sq
    l_nrm.wait()
    xm = (tok * v_nrm[...]).astype(jnp.bfloat16)
    c_br = []
    for k in range(2):
        in_copies[k].wait()
        br_buf[k, me_s] = dot(xm, v_wi[k]).astype(jnp.bfloat16)
        c_br.append(state_send(1 + k, br_buf.at[k, me_s], br_buf.at[k, me_s]))
        pending += c_br[k]
    for c in loads[1:]:
        c.wait()
    recv(c_sq)
    total = sq_buf[0]
    for j in range(1, states):
        total = total + sq_buf[j]
    inv_first = lax.rsqrt(total[:, :1] / model + NORM_EPS)
    recv(c_br[0])
    block = min(512, chans)
    for c0 in range(0, chans, block):
        cols = pl.ds(c0, block)
        value = br_buf[0, 0, :, cols].astype(jnp.float32)
        for j in range(1, states):
            value = value + br_buf[0, j, :, cols].astype(jnp.float32)
        value = value * inv_first
        conv_in[:, cols] = value
        taps = v_cs.shape[0]
        acc = v_cw[taps : taps + 1, cols] * value
        for k in range(taps):
            acc = acc + v_cw[k : k + 1, cols] * v_cs[k, :, cols]
        acc = acc + v_cb[:, cols]
        conv_out[:, cols] = acc / (1.0 + jnp.exp(-acc))
    pj_buf[me_h] = dot(conv_out[...].astype(jnp.bfloat16), v_wsp[...])
    c_pj = head_send(1, pj_buf.at[me_h], pj_buf.at[me_h])
    pending += c_pj
    out_copies = [pltpu.make_async_copy(conv_in, new_conv.at[v_cs.shape[0] - 1], o_sem.at[0])]
    for k in range(1, v_cs.shape[0]):
        out_copies.append(pltpu.make_async_copy(v_cs.at[k], new_conv.at[k - 1], o_sem.at[k]))
    for c in out_copies:
        c.start()
    recv(c_br[1])
    for c0 in range(0, chans, block):
        cols = pl.ds(c0, block)
        value = br_buf[1, 0, :, cols].astype(jnp.float32)
        for j in range(1, states):
            value = value + br_buf[1, j, :, cols].astype(jnp.float32)
        value = value * inv_first
        gate_act[:, cols] = value / (1.0 + jnp.exp(-value))
    recv(c_pj)
    projected = pj_buf[0]
    for j in range(1, heads):
        projected = projected + pj_buf[j]
    step_low = projected[:, :rank]
    step_inv = lax.rsqrt(jnp.mean(step_low * step_low, axis=1, keepdims=True) + STEP_EPS)
    step_normed = (step_low * step_inv * v_sg[...]).astype(jnp.bfloat16)
    tail = projected[:, rank:]
    lane = lax.broadcasted_iota(jnp.int32, tail.shape, 1)
    bs = []
    ks = []
    for n in range(slab):
        at = me_s * slab + n
        bs.append(jnp.sum(jnp.where(lane == at, tail, 0.0), axis=1, keepdims=True))
        ks.append(jnp.sum(jnp.where(lane == at + slab * states, tail, 0.0), axis=1, keepdims=True))
    for c0 in range(0, chans, block):
        cols = pl.ds(c0, block)
        raw = dot(step_normed, v_wst[:, cols]) + v_sb[:, cols]
        step_size = jnp.maximum(raw, 0.0) + jnp.log1p(jnp.exp(-jnp.abs(raw)))
        driven = step_size * conv_out[:, cols]
        read = None
        for n in range(slab):
            decay = jnp.exp(-step_size * jnp.exp(v_dl[n : n + 1, cols]))
            fresh = decay * v_ss[n, :, cols] + bs[n] * driven
            v_ss[n, :, cols] = fresh
            term = ks[n] * fresh
            read = term if read is None else read + term
        rd_buf[me_s, :, cols] = read.astype(jnp.bfloat16)
    c_rd = state_send(3, rd_buf.at[me_s], rd_buf.at[me_s])
    pending += c_rd
    state_out = pltpu.make_async_copy(v_ss, new_state, o_sem.at[v_cs.shape[0]])
    state_out.start()
    out_copies.append(state_out)
    recv(c_rd)
    mixed = None
    for c0 in range(0, chans, block):
        cols = pl.ds(c0, block)
        value = rd_buf[0, :, cols].astype(jnp.float32)
        for j in range(1, states):
            value = value + rd_buf[j, :, cols].astype(jnp.float32)
        act = ((value + v_sk[:, cols] * conv_out[:, cols]) * gate_act[:, cols]).astype(jnp.bfloat16)
        term = dot(act, v_wo[cols, :])
        mixed = term if mixed is None else mixed + term
    ms_buf[me_h] = mixed.astype(jnp.bfloat16)
    c_ms = head_send(2, ms_buf.at[me_h], ms_buf.at[me_h])
    pending += c_ms
    recv(c_ms)
    value = ms_buf[0].astype(jnp.float32)
    for j in range(1, heads):
        value = value + ms_buf[j].astype(jnp.float32)
    rounded = (tok + value).astype(jnp.bfloat16)
    resid[...] = rounded.astype(jnp.float32)
    rs_buf[me_s] = rounded
    c_rs = state_send(4, rs_buf.at[me_s], rs_buf.at[me_s])
    pending += c_rs
    recv(c_rs)
    rows = [rs_buf[j].astype(jnp.float32) for j in range(states)]
    square = jnp.sum(rows[0] * rows[0], axis=1, keepdims=True)
    for j in range(1, states):
        square = square + jnp.sum(rows[j] * rows[j], axis=1, keepdims=True)
    inv_second = lax.rsqrt(square / model + NORM_EPS)
    logits = None
    for j in range(states):
        cols = pl.ds(j * width, width)
        scaled = rows[j] * v_mn[:, cols]
        xn[:, cols] = (scaled * inv_second).astype(jnp.bfloat16)
        term = jnp.dot(scaled, v_rw[cols, :], precision=lax.Precision.HIGHEST, preferred_element_type=jnp.float32)
        logits = term if logits is None else logits + term
    logits = logits * inv_second
    names = lax.broadcasted_iota(jnp.int32, logits.shape, 1).astype(jnp.float32)
    hits = [names == route[:, k : k + 1] for k in range(TOPK)]
    kept = [route[:, TOPK + k : TOPK + k + 1] < CAP for k in range(TOPK)]
    chosen = [jnp.sum(jnp.where(hits[k], logits, 0.0), axis=1, keepdims=True) for k in range(TOPK)]
    token_weight = jnp.zeros_like(logits)
    loads_te = jnp.zeros_like(logits)
    for k in range(TOPK):
        gate_prob = 1.0 / (1.0 + jnp.exp(chosen[1 - k] - chosen[k]))
        token_weight = token_weight + jnp.where(hits[k] & kept[k], gate_prob, 0.0)
        loads_te = loads_te + jnp.where(hits[k] & kept[k], 1.0, 0.0)
    load_sum = jnp.sum(loads_te, axis=0, keepdims=True)
    load[...] = load_sum
    prob_mean = jnp.sum(1.0 / (1.0 + jnp.exp(-logits)), axis=0, keepdims=True) / batch
    aux[...] = experts * jnp.sum(load_sum / (batch * TOPK) * prob_mean, axis=1, keepdims=True)
    weights = []
    ids = lax.broadcasted_iota(jnp.int32, logits.shape, 1)
    for e in range(local):
        weights.append(jnp.sum(jnp.where(ids == (me_h * local + e) // split, token_weight, 0.0), axis=1, keepdims=True))
    part = v_wg.shape[2]
    hb = 256 if part % 256 == 0 else 128
    for e in range(local):
        ex_copies[e][0].wait()
        ex_copies[e][1].wait()

        def hidden_step(i, carry):
            cols = pl.ds(pl.multiple_of(i * hb, hb), hb)
            gate_val = dot(xn[...], v_wg[e, :, cols])
            up_val = dot(xn[...], v_wu[e, :, cols])
            hid[e, :, cols] = (gate_val / (1.0 + jnp.exp(-gate_val)) * up_val).astype(jnp.bfloat16)
            return carry

        lax.fori_loop(0, part // hb, hidden_step, 0)
    for e in range(local):
        ex_copies[e][2].wait()
    c_x = []
    for ds in range(states):
        dest_s = lax.rem(me_s + ds + 1, states)
        cols = pl.ds(pl.multiple_of(dest_s * width, width), width)
        mix = None
        for e in range(local):
            term = weights[e] * dot(hid[e], v_wd[e, :, cols])
            mix = term if mix is None else mix + term
        for h in range(heads):
            xo_buf[ds * heads + h] = mix[h * own : (h + 1) * own].astype(xo_buf.dtype)
        slot = me_s * heads + me_h
        for dh in range(1, heads + 1):
            dest_h = lax.rem(me_h + dh, heads)
            if ds == states - 1 and dh == heads:
                continue
            c = pltpu.make_async_remote_copy(
                src_ref=xo_buf.at[ds * heads + dest_h],
                dst_ref=xi_buf.at[slot],
                send_sem=x_send.at[ds * heads + dh - 1],
                recv_sem=x_recv.at[ds * heads + dh - 1],
                device_id={"head": dest_h, "state": dest_s},
                device_id_type=pl.DeviceIdType.MESH,
            )
            c.start()
            c_x.append(c)
    xi_buf[me_s * heads + me_h] = xo_buf[(states - 1) * heads + me_h]
    base = jnp.zeros(out.shape, jnp.float32)
    for h in range(heads):
        base = base + jnp.where(me_h == h, resid[h * own : (h + 1) * own], 0.0)
    recv(c_x)
    mix = xi_buf[0].astype(jnp.float32)
    for j in range(1, heads * states):
        mix = mix + xi_buf[j].astype(jnp.float32)
    out[...] = (base + mix).astype(jnp.bfloat16)
    for c in pending + c_x:
        c.wait_send()
    for c in out_copies:
        c.wait()


def fused_device(tokens, mixer_norm, input_proj, conv_weight, conv_bias, conv_state, state_proj, step_gain, step_proj, step_bias, decay_log, skip_gain, ssm_state, output_proj, moe_norm, router_weight, expert_ids, slot_ids, gate_proj, up_proj, down_proj):
    heads = lax.axis_size("head")
    states = lax.axis_size("state")
    own, width = tokens.shape
    batch = own * heads
    local, model, part = gate_proj.shape
    experts = router_weight.shape[1]
    split = heads * local // experts
    slab = decay_log.shape[0]
    chans = conv_bias.shape[0]
    lanes = 128
    route = jnp.concatenate([expert_ids, slot_ids], axis=1).astype(jnp.bfloat16)
    route = jnp.pad(route, ((0, 0), (0, lanes - route.shape[1])))
    pay = jnp.concatenate([tokens, route], axis=1)
    mine = jnp.arange(batch)[:, None] // own == lax.axis_index("head")
    pay = jnp.where(mine, jnp.tile(pay, (heads, 1)), 0)
    row = lambda a: a.reshape(1, -1)
    args = [pay, row(mixer_norm), input_proj, conv_weight, row(conv_bias), conv_state, state_proj, row(step_gain), step_proj, row(step_bias), decay_log, row(skip_gain), ssm_state, output_proj, row(moe_norm), router_weight, gate_proj, up_proj, down_proj]
    f32, bf16 = jnp.float32, jnp.bfloat16
    order = [1, 2, 3, 4, 5, 6, 7, 8, 9, 10, 11, 12, 13, 14, 15, 16, 17, 18]
    scratch = [pltpu.VMEM(args[i].shape, args[i].dtype) for i in order]
    scratch += [
        pltpu.VMEM((heads,) + pay.shape, bf16),
        pltpu.VMEM((states, batch, lanes), f32),
        pltpu.VMEM((2, states, batch, chans), bf16),
        pltpu.VMEM((heads, batch, state_proj.shape[1]), f32),
        pltpu.VMEM((states, batch, chans), bf16),
        pltpu.VMEM((heads, batch, width), bf16),
        pltpu.VMEM((states, batch, width), bf16),
        pltpu.VMEM((heads * states, own, width), f32),
        pltpu.VMEM((heads * states, own, width), f32),
        pltpu.VMEM((batch, chans), f32),
        pltpu.VMEM((batch, chans), f32),
        pltpu.VMEM((batch, chans), f32),
        pltpu.VMEM((batch, width), f32),
        pltpu.VMEM((batch, model), bf16),
        pltpu.VMEM((local, batch, part), bf16),
        pltpu.SemaphoreType.DMA((14,)),
        pltpu.SemaphoreType.DMA((3 * local,)),
        pltpu.SemaphoreType.DMA((2,)),
        pltpu.SemaphoreType.DMA((3, heads)),
        pltpu.SemaphoreType.DMA((3, heads)),
        pltpu.SemaphoreType.DMA((5, states)),
        pltpu.SemaphoreType.DMA((5, states)),
        pltpu.SemaphoreType.DMA((heads * states,)),
        pltpu.SemaphoreType.DMA((heads * states,)),
        pltpu.SemaphoreType.DMA((conv_state.shape[0] + 1,)),
    ]
    anywhere = pl.BlockSpec(memory_space=pl.ANY)
    vmem = pl.BlockSpec(memory_space=pltpu.VMEM)
    layer_out, new_conv, new_state, load, aux = pl.pallas_call(
        lambda *refs: fused_kernel((heads, states, own, local, split, slab), *refs),
        out_shape=[
            jax.ShapeDtypeStruct(tokens.shape, bf16),
            jax.ShapeDtypeStruct(conv_state.shape, f32),
            jax.ShapeDtypeStruct(ssm_state.shape, f32),
            jax.ShapeDtypeStruct((1, experts), f32),
            jax.ShapeDtypeStruct((1, 1), f32),
        ],
        in_specs=[vmem] + [anywhere] * 18,
        out_specs=[vmem, anywhere, anywhere, vmem, vmem],
        scratch_shapes=scratch,
        compiler_params=pltpu.CompilerParams(collective_id=0, has_side_effects=True, vmem_limit_bytes=VMEM_BYTES),
        name="decode",
    )(*args)
    return (layer_out, new_conv, new_state, load.reshape(-1), aux.reshape(1))


def per_device_any(*args):
    gate_proj = args[18]
    batch = args[0].shape[0] * lax.axis_size("head")
    held = sum(args[i].size * args[i].dtype.itemsize for i in (2, 6, 8, 12, 13, 18, 19, 20))
    if batch <= 64 and gate_proj.shape[2] % 128 == 0 and held < VMEM_BYTES * 7 // 8:
        return fused_device(*args)
    return per_device(*args)


def solution(mesh):
    return jax.shard_map(
        per_device_any,
        mesh=mesh,
        in_specs=(
            P(("groups", "head"), "state"),
            P("state"),
            P(None, "state", "head"),
            P(None, "head"),
            P("head"),
            P(None, "groups", "head"),
            P("head", None),
            P(),
            P(None, "head"),
            P("head"),
            P("state", "head"),
            P("head"),
            P("state", "groups", "head"),
            P("head", "state"),
            P(),
            P(),
            P(("groups", "head"), None),
            P(("groups", "head"), None),
            P("head", None, "state"),
            P("head", None, "state"),
            P("head", "state", None),
        ),
        out_specs=(
            P(("groups", "head"), "state"),
            P(None, "groups", "head"),
            P("state", "groups", "head"),
            P("groups"),
            P("groups"),
        ),
        check_vma=False,
    )
```

```python
import jax
import jax.numpy as jnp
from jax import lax
from jax.experimental import pallas as pl
from jax.experimental.pallas import tpu as pltpu
from jax.sharding import PartitionSpec as P

D = 2048
D_STATE = 16
DT_RANK = 256
EXPERTS = 8
TOPK = 2
CAP = 2


NORM_EPS = 1e-05
STEP_EPS = 1e-06
VMEM_BYTES = 67043328


def expert_ffn(received, gate_proj, up_proj, down_proj):
    gate_val = jnp.einsum("nlcd,ldf->nlcf", received, gate_proj, preferred_element_type=jnp.float32)
    up_val = jnp.einsum("nlcd,ldf->nlcf", received, up_proj, preferred_element_type=jnp.float32)
    hidden = (jax.nn.silu(gate_val) * up_val).astype(jnp.bfloat16)
    return jnp.einsum("nlcf,lfd->nlcd", hidden, down_proj, preferred_element_type=jnp.float32)


def per_device(
    tokens,
    mixer_norm,
    input_proj,
    conv_weight,
    conv_bias,
    conv_state,
    state_proj,
    step_gain,
    step_proj,
    step_bias,
    decay_log,
    skip_gain,
    ssm_state,
    output_proj,
    moe_norm,
    router_weight,
    expert_ids,
    slot_ids,
    gate_proj,
    up_proj,
    down_proj,
):
    head_count = lax.axis_size("head")
    state_index = lax.axis_index("state")
    own_rows = tokens.shape[0]
    tok_f32 = tokens.astype(jnp.float32)
    first_sq = lax.psum(jnp.sum(tok_f32 * tok_f32, axis=1), "state")
    inv_first = lax.rsqrt(first_sq / D + NORM_EPS)[:, None]
    normed = (tok_f32 * inv_first * mixer_norm).astype(jnp.bfloat16)
    branch_part = jnp.einsum(
        "td,kdc->ktc",
        lax.all_gather(normed, "head", axis=0, tiled=True),
        input_proj,
        preferred_element_type=jnp.float32,
    )
    branch_full = lax.psum(branch_part, "state")
    conv_input = branch_full[0]
    gate_branch = branch_full[1]
    window = jnp.concatenate([conv_state, conv_input[None]], axis=0)
    conv_out = jax.nn.silu(jnp.sum(conv_weight[:, None, :] * window, axis=0) + conv_bias)
    new_conv = window[1:]
    proj_part = jnp.dot(
        conv_out.astype(jnp.bfloat16), state_proj, preferred_element_type=jnp.float32
    )
    projected = lax.psum(proj_part, "head")
    step_low = projected[:, :DT_RANK]
    state_slab = decay_log.shape[0]
    b_input = lax.dynamic_slice_in_dim(projected, DT_RANK + state_index * state_slab, state_slab, 1)
    c_output = lax.dynamic_slice_in_dim(
        projected, DT_RANK + D_STATE + state_index * state_slab, state_slab, 1
    )
    step_inv = lax.rsqrt(jnp.mean(step_low * step_low, axis=1, keepdims=True) + STEP_EPS)
    step_normed = (step_low * step_inv * step_gain).astype(jnp.bfloat16)
    step_size = jax.nn.softplus(
        jnp.dot(step_normed, step_proj, preferred_element_type=jnp.float32) + step_bias
    )
    decay_rate = jnp.exp(-step_size[None] * jnp.exp(decay_log)[:, None, :])
    new_state = decay_rate * ssm_state + step_size[None] * b_input.T[:, :, None] * conv_out[None]
    read_part = jnp.sum(c_output.T[:, :, None] * new_state, axis=0)
    readout = lax.psum(read_part, "state")
    mixer_act = ((readout + skip_gain * conv_out) * jax.nn.silu(gate_branch)).astype(jnp.bfloat16)
    mixer_sum = lax.psum_scatter(
        jnp.dot(mixer_act, output_proj, preferred_element_type=jnp.float32),
        "head",
        scatter_dimension=0,
        tiled=True,
    )
    residual = (tok_f32 + mixer_sum).astype(jnp.bfloat16)
    full_rows = lax.all_gather(residual, "state", axis=1, tiled=True).astype(jnp.float32)
    inv_second = lax.rsqrt(jnp.mean(full_rows * full_rows, axis=1, keepdims=True) + NORM_EPS)
    scaled = full_rows * moe_norm
    logits = inv_second * jnp.dot(scaled, router_weight, precision=lax.Precision.HIGHEST)
    row_normed = (scaled * inv_second).astype(jnp.bfloat16)
    expert_hit = expert_ids[:, :, None] == jnp.arange(EXPERTS, dtype=jnp.int32)[None, None, :]
    chosen = jnp.sum(jnp.where(expert_hit, logits[:, None, :], 0.0), axis=2)
    gate_probs = jax.nn.sigmoid(chosen - chosen[:, ::-1])
    kept_mask = slot_ids < CAP
    mix_weight = jnp.where(kept_mask, gate_probs, 0.0)
    slot_hit = slot_ids[:, :, None] == jnp.arange(CAP, dtype=jnp.int32)[None, None, :]
    slot_place = expert_hit[:, :, :, None] & slot_hit[:, :, None, :]
    dispatch = jnp.sum(slot_place.astype(jnp.int32), axis=1).astype(jnp.bfloat16)
    combine_weight = jnp.sum(jnp.where(slot_place, mix_weight[:, :, None, None], 0.0), axis=1)
    outgoing = jnp.einsum(
        "tec,td->ecd", dispatch, row_normed, preferred_element_type=jnp.float32
    ).astype(jnp.bfloat16)
    row_width = outgoing.shape[2]
    local_experts = gate_proj.shape[0]
    expert_groups = EXPERTS // local_experts
    copies = head_count * local_experts // EXPERTS
    outgoing = jnp.broadcast_to(
        outgoing.reshape(expert_groups, 1, local_experts, CAP, row_width),
        (expert_groups, copies, local_experts, CAP, row_width),
    )
    outgoing = outgoing.reshape(head_count, local_experts, CAP, row_width)
    partial_out = expert_ffn(
        lax.all_to_all(outgoing, "head", split_axis=0, concat_axis=0, tiled=True),
        gate_proj,
        up_proj,
        down_proj,
    )
    returned = lax.all_to_all(
        partial_out.astype(jnp.bfloat16), "head", split_axis=0, concat_axis=0, tiled=True
    ).astype(partial_out.dtype)
    per_expert = returned.reshape(expert_groups, copies, local_experts, CAP, row_width).sum(axis=1)
    per_expert = per_expert.reshape(EXPERTS, CAP, row_width)
    expert_mix = jnp.einsum(
        "tec,ecd->td", combine_weight, per_expert, precision=lax.Precision.HIGHEST
    )
    expert_mix = lax.psum_scatter(
        expert_mix.astype(jnp.bfloat16), "state", scatter_dimension=1, tiled=True
    ).astype(jnp.float32)
    layer_out = (residual.astype(jnp.float32) + expert_mix).astype(jnp.bfloat16)
    load_own = jnp.sum(jnp.where(expert_hit & kept_mask[:, :, None], 1.0, 0.0), axis=(0, 1)).astype(
        jnp.float32
    )
    prob_own = jnp.sum(jax.nn.sigmoid(logits), axis=0)
    load_sum, prob_sum = lax.psum((load_own, prob_own), "head")
    total_rows = head_count * own_rows
    aux_value = EXPERTS * jnp.sum(load_sum / (total_rows * TOPK) * (prob_sum / total_rows))
    return (layer_out, new_conv, new_state, load_sum, aux_value.reshape(1))


def dot(left, right):
    return jnp.dot(left, right, preferred_element_type=jnp.float32)


def dot_t(left, right, precision=None):
    return lax.dot_general(left, right, (((1,), (1,)), ((), ())), precision=precision, preferred_element_type=jnp.float32)


def fused_kernel(dims, *refs):
    heads, states, own, local, split, slab = dims
    (pay, nrm, wi, cw, cb, cs, wsp, sg, wst, sb, dl, sk, ss, wo, mn, rw, wg, wu, wd) = refs[:19]
    (out, new_conv, new_state, load, aux) = refs[19:24]
    (v_nrm, v_wi, v_cw, v_cb, v_cs, v_wsp, v_sg, v_wst, v_sb, v_dl, v_sk, v_ss, v_wo, v_mn, v_rw, v_wg, v_wu, v_wd) = refs[24:42]
    (pay_buf, sq_buf, br_buf, pj_buf, rd_buf, ms_buf, rs_buf, xo_buf, xi_buf) = refs[42:51]
    (conv_in, conv_out, gate_act, resid, xn, hid, ld_sem, ex_sem, in_sem, h_send, h_recv, s_send, s_recv, x_send, x_recv, o_sem) = refs[51:]
    me_h = lax.axis_index("head")
    me_s = lax.axis_index("state")
    batch = pay.shape[0]
    width = v_nrm.shape[1]
    model = width * states
    chans = v_cb.shape[1]
    rank = v_sg.shape[1]
    experts = v_rw.shape[0]

    smalls = [(nrm, v_nrm), (cw, v_cw), (cb, v_cb), (cs, v_cs), (wsp, v_wsp), (sg, v_sg), (wst, v_wst), (sb, v_sb), (dl, v_dl), (sk, v_sk), (ss, v_ss), (wo, v_wo), (mn, v_mn), (rw, v_rw)]
    in_copies = [pltpu.make_async_copy(wi.at[k], v_wi.at[k], in_sem.at[k]) for k in range(2)]
    loads = [pltpu.make_async_copy(a, b, ld_sem.at[i]) for i, (a, b) in enumerate(smalls)]
    (l_nrm, l_cw, l_cb, l_cs, l_wsp, l_sg, l_wst, l_sb, l_dl, l_sk, l_ss, l_wo, l_mn, l_rw) = loads
    ex_copies = []
    for e in range(local):
        ex_copies.append([pltpu.make_async_copy(a.at[e], b.at[e], ex_sem.at[3 * e + j]) for j, (a, b) in enumerate(((wg, v_wg), (wu, v_wu), (wd, v_wd)))])
    l_nrm.start()
    for c in in_copies:
        c.start()
    for c in loads[1:]:
        c.start()

    barrier = pltpu.get_barrier_semaphore()
    for dh in range(heads):
        for ds in range(states):
            if dh or ds:
                pl.semaphore_signal(
                    barrier,
                    inc=1,
                    device_id={"head": lax.rem(me_h + dh, heads), "state": lax.rem(me_s + ds, states)},
                    device_id_type=pl.DeviceIdType.MESH,
                )
    pl.semaphore_wait(barrier, heads * states - 1)

    def head_send(step, source, dest):
        copies = []
        for d in range(1, heads):
            c = pltpu.make_async_remote_copy(
                src_ref=source,
                dst_ref=dest,
                send_sem=h_send.at[step, d],
                recv_sem=h_recv.at[step, d],
                device_id={"head": lax.rem(me_h + d, heads)},
                device_id_type=pl.DeviceIdType.MESH,
            )
            c.start()
            copies.append(c)
        return copies

    def state_send(step, source, dest):
        copies = []
        for d in range(1, states):
            c = pltpu.make_async_remote_copy(
                src_ref=source,
                dst_ref=dest,
                send_sem=s_send.at[step, d],
                recv_sem=s_recv.at[step, d],
                device_id={"state": lax.rem(me_s + d, states)},
                device_id_type=pl.DeviceIdType.MESH,
            )
            c.start()
            copies.append(c)
        return copies

    def recv(copies):
        for c in copies:
            c.wait_recv()

    pending = []
    c_pay = head_send(0, pay, pay_buf.at[me_h])
    pending += c_pay
    pay_buf[me_h] = pay[...]
    for group in ex_copies:
        for c in group:
            c.start()
    recv(c_pay)
    whole = pay_buf[0].astype(jnp.float32)
    for j in range(1, heads):
        whole = whole + pay_buf[j].astype(jnp.float32)
    tok = whole[:, :width]
    route = whole[:, width:]
    sq_buf[me_s] = jnp.broadcast_to(jnp.sum(tok * tok, axis=1, keepdims=True), sq_buf.shape[1:])
    c_sq = state_send(0, sq_buf.at[me_s], sq_buf.at[me_s])
    pending += c_sq
    l_nrm.wait()
    xm = (tok * v_nrm[...]).astype(jnp.bfloat16)
    c_br = []
    for k in range(2):
        in_copies[k].wait()
        br_buf[k, me_s] = dot(xm, v_wi[k]).astype(jnp.bfloat16)
        c_br.append(state_send(1 + k, br_buf.at[k, me_s], br_buf.at[k, me_s]))
        pending += c_br[k]
    for c in loads[1:]:
        c.wait()
    recv(c_sq)
    total = sq_buf[0]
    for j in range(1, states):
        total = total + sq_buf[j]
    inv_first = lax.rsqrt(total[:, :1] / model + NORM_EPS)
    recv(c_br[0])
    block = min(512, chans)
    for c0 in range(0, chans, block):
        cols = pl.ds(c0, block)
        value = br_buf[0, 0, :, cols].astype(jnp.float32)
        for j in range(1, states):
            value = value + br_buf[0, j, :, cols].astype(jnp.float32)
        value = value * inv_first
        conv_in[:, cols] = value
        taps = v_cs.shape[0]
        acc = v_cw[taps : taps + 1, cols] * value
        for k in range(taps):
            acc = acc + v_cw[k : k + 1, cols] * v_cs[k, :, cols]
        acc = acc + v_cb[:, cols]
        conv_out[:, cols] = acc / (1.0 + jnp.exp(-acc))
    pj_buf[me_h] = dot_t(conv_out[...].astype(jnp.bfloat16), v_wsp[...])
    c_pj = head_send(1, pj_buf.at[me_h], pj_buf.at[me_h])
    pending += c_pj
    out_copies = [pltpu.make_async_copy(conv_in, new_conv.at[v_cs.shape[0] - 1], o_sem.at[0])]
    for k in range(1, v_cs.shape[0]):
        out_copies.append(pltpu.make_async_copy(v_cs.at[k], new_conv.at[k - 1], o_sem.at[k]))
    for c in out_copies:
        c.start()
    recv(c_br[1])
    for c0 in range(0, chans, block):
        cols = pl.ds(c0, block)
        value = br_buf[1, 0, :, cols].astype(jnp.float32)
        for j in range(1, states):
            value = value + br_buf[1, j, :, cols].astype(jnp.float32)
        value = value * inv_first
        gate_act[:, cols] = value / (1.0 + jnp.exp(-value))
    recv(c_pj)
    projected = pj_buf[0]
    for j in range(1, heads):
        projected = projected + pj_buf[j]
    step_low = projected[:, :rank]
    step_inv = lax.rsqrt(jnp.mean(step_low * step_low, axis=1, keepdims=True) + STEP_EPS)
    step_normed = (step_low * step_inv * v_sg[...]).astype(jnp.bfloat16)
    tail = projected[:, rank:]
    lane = lax.broadcasted_iota(jnp.int32, tail.shape, 1)
    bs = []
    ks = []
    for n in range(slab):
        at = me_s * slab + n
        bs.append(jnp.sum(jnp.where(lane == at, tail, 0.0), axis=1, keepdims=True))
        ks.append(jnp.sum(jnp.where(lane == at + slab * states, tail, 0.0), axis=1, keepdims=True))
    for c0 in range(0, chans, block):
        cols = pl.ds(c0, block)
        raw = dot(step_normed, v_wst[:, cols]) + v_sb[:, cols]
        step_size = jnp.maximum(raw, 0.0) + jnp.log1p(jnp.exp(-jnp.abs(raw)))
        driven = step_size * conv_out[:, cols]
        read = None
        for n in range(slab):
            decay = jnp.exp(-step_size * jnp.exp(v_dl[n : n + 1, cols]))
            fresh = decay * v_ss[n, :, cols] + bs[n] * driven
            v_ss[n, :, cols] = fresh
            term = ks[n] * fresh
            read = term if read is None else read + term
        rd_buf[me_s, :, cols] = read.astype(jnp.bfloat16)
    c_rd = state_send(3, rd_buf.at[me_s], rd_buf.at[me_s])
    pending += c_rd
    state_out = pltpu.make_async_copy(v_ss, new_state, o_sem.at[v_cs.shape[0]])
    state_out.start()
    out_copies.append(state_out)
    recv(c_rd)
    mixed = None
    for c0 in range(0, chans, block):
        cols = pl.ds(c0, block)
        value = rd_buf[0, :, cols].astype(jnp.float32)
        for j in range(1, states):
            value = value + rd_buf[j, :, cols].astype(jnp.float32)
        act = ((value + v_sk[:, cols] * conv_out[:, cols]) * gate_act[:, cols]).astype(jnp.bfloat16)
        term = dot(act, v_wo[cols, :])
        mixed = term if mixed is None else mixed + term
    ms_buf[me_h] = mixed.astype(jnp.bfloat16)
    c_ms = head_send(2, ms_buf.at[me_h], ms_buf.at[me_h])
    pending += c_ms
    recv(c_ms)
    value = ms_buf[0].astype(jnp.float32)
    for j in range(1, heads):
        value = value + ms_buf[j].astype(jnp.float32)
    rounded = (tok + value).astype(jnp.bfloat16)
    resid[...] = rounded.astype(jnp.float32)
    rs_buf[me_s] = rounded
    c_rs = state_send(4, rs_buf.at[me_s], rs_buf.at[me_s])
    pending += c_rs
    recv(c_rs)
    rows = [rs_buf[j].astype(jnp.float32) for j in range(states)]
    square = jnp.sum(rows[0] * rows[0], axis=1, keepdims=True)
    for j in range(1, states):
        square = square + jnp.sum(rows[j] * rows[j], axis=1, keepdims=True)
    inv_second = lax.rsqrt(square / model + NORM_EPS)
    logits = None
    for j in range(states):
        cols = pl.ds(j * width, width)
        scaled = rows[j] * v_mn[:, cols]
        xn[:, cols] = (scaled * inv_second).astype(jnp.bfloat16)
        term = dot_t(scaled, v_rw[:, cols], lax.Precision.HIGHEST)
        logits = term if logits is None else logits + term
    logits = logits * inv_second
    names = lax.broadcasted_iota(jnp.int32, logits.shape, 1).astype(jnp.float32)
    hits = [names == route[:, k : k + 1] for k in range(TOPK)]
    kept = [route[:, TOPK + k : TOPK + k + 1] < CAP for k in range(TOPK)]
    chosen = [jnp.sum(jnp.where(hits[k], logits, 0.0), axis=1, keepdims=True) for k in range(TOPK)]
    token_weight = jnp.zeros_like(logits)
    loads_te = jnp.zeros_like(logits)
    for k in range(TOPK):
        gate_prob = 1.0 / (1.0 + jnp.exp(chosen[1 - k] - chosen[k]))
        token_weight = token_weight + jnp.where(hits[k] & kept[k], gate_prob, 0.0)
        loads_te = loads_te + jnp.where(hits[k] & kept[k], 1.0, 0.0)
    load_sum = jnp.sum(loads_te, axis=0, keepdims=True)
    load[...] = load_sum
    prob_mean = jnp.sum(1.0 / (1.0 + jnp.exp(-logits)), axis=0, keepdims=True) / batch
    aux[...] = experts * jnp.sum(load_sum / (batch * TOPK) * prob_mean, axis=1, keepdims=True)
    weights = []
    ids = lax.broadcasted_iota(jnp.int32, logits.shape, 1)
    for e in range(local):
        weights.append(jnp.sum(jnp.where(ids == (me_h * local + e) // split, token_weight, 0.0), axis=1, keepdims=True))
    part = v_wg.shape[2]
    hb = 256 if part % 256 == 0 else 128
    for e in range(local):
        ex_copies[e][0].wait()
        ex_copies[e][1].wait()

        def hidden_step(i, carry):
            cols = pl.ds(pl.multiple_of(i * hb, hb), hb)
            gate_val = dot(xn[...], v_wg[e, :, cols])
            up_val = dot(xn[...], v_wu[e, :, cols])
            hid[e, :, cols] = (gate_val / (1.0 + jnp.exp(-gate_val)) * up_val).astype(jnp.bfloat16)
            return carry

        lax.fori_loop(0, part // hb, hidden_step, 0)
    for e in range(local):
        ex_copies[e][2].wait()
    c_x = []
    for ds in range(states):
        dest_s = lax.rem(me_s + ds + 1, states)
        cols = pl.ds(pl.multiple_of(dest_s * width, width), width)
        mix = None
        for e in range(local):
            term = weights[e] * dot(hid[e], v_wd[e, :, cols])
            mix = term if mix is None else mix + term
        for h in range(heads):
            xo_buf[ds * heads + h] = mix[h * own : (h + 1) * own].astype(xo_buf.dtype)
        slot = me_s * heads + me_h
        for dh in range(1, heads + 1):
            dest_h = lax.rem(me_h + dh, heads)
            if ds == states - 1 and dh == heads:
                continue
            c = pltpu.make_async_remote_copy(
                src_ref=xo_buf.at[ds * heads + dest_h],
                dst_ref=xi_buf.at[slot],
                send_sem=x_send.at[ds * heads + dh - 1],
                recv_sem=x_recv.at[ds * heads + dh - 1],
                device_id={"head": dest_h, "state": dest_s},
                device_id_type=pl.DeviceIdType.MESH,
            )
            c.start()
            c_x.append(c)
    xi_buf[me_s * heads + me_h] = xo_buf[(states - 1) * heads + me_h]
    base = jnp.zeros(out.shape, jnp.float32)
    for h in range(heads):
        base = base + jnp.where(me_h == h, resid[h * own : (h + 1) * own], 0.0)
    recv(c_x)
    mix = xi_buf[0].astype(jnp.float32)
    for j in range(1, heads * states):
        mix = mix + xi_buf[j].astype(jnp.float32)
    out[...] = (base + mix).astype(jnp.bfloat16)
    for c in pending + c_x:
        c.wait_send()
    for c in out_copies:
        c.wait()


def fused_device(tokens, mixer_norm, input_proj, conv_weight, conv_bias, conv_state, state_proj, step_gain, step_proj, step_bias, decay_log, skip_gain, ssm_state, output_proj, moe_norm, router_weight, expert_ids, slot_ids, gate_proj, up_proj, down_proj):
    heads = lax.axis_size("head")
    states = lax.axis_size("state")
    own, width = tokens.shape
    batch = own * heads
    local, model, part = gate_proj.shape
    experts = router_weight.shape[1]
    split = heads * local // experts
    slab = decay_log.shape[0]
    chans = conv_bias.shape[0]
    lanes = 128
    route = jnp.concatenate([expert_ids, slot_ids], axis=1).astype(jnp.bfloat16)
    route = jnp.pad(route, ((0, 0), (0, lanes - route.shape[1])))
    pay = jnp.concatenate([tokens, route], axis=1)
    mine = jnp.arange(batch)[:, None] // own == lax.axis_index("head")
    pay = jnp.where(mine, jnp.tile(pay, (heads, 1)), 0)
    row = lambda a: a.reshape(1, -1)
    args = [pay, row(mixer_norm), input_proj, conv_weight, row(conv_bias), conv_state, state_proj.T, row(step_gain), step_proj, row(step_bias), decay_log, row(skip_gain), ssm_state, output_proj, row(moe_norm), router_weight.T, gate_proj, up_proj, down_proj]
    f32, bf16 = jnp.float32, jnp.bfloat16
    order = [1, 2, 3, 4, 5, 6, 7, 8, 9, 10, 11, 12, 13, 14, 15, 16, 17, 18]
    scratch = [pltpu.VMEM(args[i].shape, args[i].dtype) for i in order]
    scratch += [
        pltpu.VMEM((heads,) + pay.shape, bf16),
        pltpu.VMEM((states, batch, lanes), f32),
        pltpu.VMEM((2, states, batch, chans), bf16),
        pltpu.VMEM((heads, batch, state_proj.shape[1]), f32),
        pltpu.VMEM((states, batch, chans), bf16),
        pltpu.VMEM((heads, batch, width), bf16),
        pltpu.VMEM((states, batch, width), bf16),
        pltpu.VMEM((heads * states, own, width), f32),
        pltpu.VMEM((heads * states, own, width), f32),
        pltpu.VMEM((batch, chans), f32),
        pltpu.VMEM((batch, chans), f32),
        pltpu.VMEM((batch, chans), f32),
        pltpu.VMEM((batch, width), f32),
        pltpu.VMEM((batch, model), bf16),
        pltpu.VMEM((local, batch, part), bf16),
        pltpu.SemaphoreType.DMA((14,)),
        pltpu.SemaphoreType.DMA((3 * local,)),
        pltpu.SemaphoreType.DMA((2,)),
        pltpu.SemaphoreType.DMA((3, heads)),
        pltpu.SemaphoreType.DMA((3, heads)),
        pltpu.SemaphoreType.DMA((5, states)),
        pltpu.SemaphoreType.DMA((5, states)),
        pltpu.SemaphoreType.DMA((heads * states,)),
        pltpu.SemaphoreType.DMA((heads * states,)),
        pltpu.SemaphoreType.DMA((conv_state.shape[0] + 1,)),
    ]
    anywhere = pl.BlockSpec(memory_space=pl.ANY)
    vmem = pl.BlockSpec(memory_space=pltpu.VMEM)
    layer_out, new_conv, new_state, load, aux = pl.pallas_call(
        lambda *refs: fused_kernel((heads, states, own, local, split, slab), *refs),
        out_shape=[
            jax.ShapeDtypeStruct(tokens.shape, bf16),
            jax.ShapeDtypeStruct(conv_state.shape, f32),
            jax.ShapeDtypeStruct(ssm_state.shape, f32),
            jax.ShapeDtypeStruct((1, experts), f32),
            jax.ShapeDtypeStruct((1, 1), f32),
        ],
        in_specs=[vmem] + [anywhere] * 18,
        out_specs=[vmem, anywhere, anywhere, vmem, vmem],
        scratch_shapes=scratch,
        compiler_params=pltpu.CompilerParams(collective_id=0, has_side_effects=True, vmem_limit_bytes=VMEM_BYTES),
        name="decode",
    )(*args)
    return (layer_out, new_conv, new_state, load.reshape(-1), aux.reshape(1))


def per_device_any(*args):
    gate_proj = args[18]
    batch = args[0].shape[0] * lax.axis_size("head")
    held = sum(args[i].size * args[i].dtype.itemsize for i in (2, 6, 8, 12, 13, 18, 19, 20))
    if batch <= 64 and gate_proj.shape[2] % 128 == 0 and held < VMEM_BYTES * 7 // 8:
        return fused_device(*args)
    return per_device(*args)


def solution(mesh):
    return jax.shard_map(
        per_device_any,
        mesh=mesh,
        in_specs=(
            P(("groups", "head"), "state"),
            P("state"),
            P(None, "state", "head"),
            P(None, "head"),
            P("head"),
            P(None, "groups", "head"),
            P("head", None),
            P(),
            P(None, "head"),
            P("head"),
            P("state", "head"),
            P("head"),
            P("state", "groups", "head"),
            P("head", "state"),
            P(),
            P(),
            P(("groups", "head"), None),
            P(("groups", "head"), None),
            P("head", None, "state"),
            P("head", None, "state"),
            P("head", "state", None),
        ),
        out_specs=(
            P(("groups", "head"), "state"),
            P(None, "groups", "head"),
            P("state", "groups", "head"),
            P("groups"),
            P("groups"),
        ),
        check_vma=False,
    )
```
